32 devices in a mesh: fft: 16 (over z, x, core), band: 2 (over y).
Axes of the slice: x: 2, y: 2, z: 4, core: 2. Of those that a mesh axis runs over, the one named last changes fastest.
Arguments:
- wavefunctions: float32 [2, 4, 128, 128, 128], P(None, 'band', 'fft'), may hold values from -6 to 6
- potential: float32 [128, 128, 128], P('fft'), may hold values from -30 to 10
- occupation: float32 [4], P('band'), may hold values from 0.05 to 1
Outputs:
- propagated: float32 [2, 4, 128, 128, 128], P(None, 'band', 'fft')
- reduced_gradient: float32 [128, 128, 128], P('fft', 'band')
- exchange_density: float32 [128, 128, 128], P('fft', 'band')
The draws below stay inside these ranges and needn't reach their ends.
All inputs are finite; a program needn't handle non-finite values.
Results may differ from the reference program's by a relative error of at most 0.0003.
Values sent between devices are 32-bit elements; how exact they have to be, the bound alone decides.
A program may use at most 64 MiB of HBM per device.

```python
import math
import jax
import jax.numpy as jnp
from jax import lax

GRID = 128
BANDS = 4


def draw_wavefunctions(key, part):
    shape_envelope = (2, BANDS, 1, GRID, GRID)
    shape_whole = (2, BANDS, GRID, GRID, GRID)
    planes = jnp.arange(GRID, dtype=jnp.int32)
    alternate = (1 - 2 * (planes % 2)).astype(jnp.float32)[None, None, :, None, None]
    phase_angle = planes.astype(jnp.float32) * (2.0 * math.pi / GRID)
    cosine = jnp.cos(phase_angle)[None, None, :, None, None]
    sine_wave = jnp.sin(phase_angle)[None, None, :, None, None]
    first_key = jax.random.fold_in(key, 11)
    second_key = jax.random.fold_in(key, 12)
    third_key = jax.random.fold_in(key, 13)
    fourth_key = jax.random.fold_in(key, 14)
    offset_part = 0.7 * jax.random.normal(first_key, shape_envelope, jnp.float32)
    swing_cos = 0.7 * jax.random.normal(second_key, shape_envelope, jnp.float32)
    swing_sin = 0.7 * jax.random.normal(third_key, shape_envelope, jnp.float32)
    rough_part = 0.35 * jax.random.normal(fourth_key, shape_whole, jnp.float32)
    envelope = offset_part + swing_cos * cosine + swing_sin * sine_wave
    values = alternate * envelope + rough_part
    return jnp.clip(values, -6.0, 6.0).astype(jnp.float32)


def draw_potential(key, part):
    side_key = jax.random.fold_in(key, 31)
    depth_key = jax.random.fold_in(key, 32)
    chosen = jax.random.bernoulli(side_key, 0.5, (GRID, GRID, GRID))
    sides = jnp.where(chosen, 1.0, -1.0).astype(jnp.float32)
    spread = jax.random.uniform(depth_key, (GRID, GRID, GRID), jnp.float32, 0.0, 1.0)
    depth = 0.6 + 0.4 * spread
    return (-10.0 + 20.0 * sides * depth).astype(jnp.float32)


def shard_levels(stream_key, shape, split, low, largest):
    def one(dim, blocks):
        heights = jax.random.uniform(jax.random.fold_in(jax.random.fold_in(stream_key, 6), dim), (blocks,), jnp.float32, low / len(split), largest / len(split))
        return jnp.repeat(jnp.exp(heights), shape[dim] // blocks).reshape((-1,) + (1,) * (len(shape) - dim - 1))

    gain = one(*split[0])
    for cut in split[1:]:
        gain = gain * one(*cut)
    return gain


def setup_inputs(seed: int = 0) -> dict:
    key_of = jax.random.split(jax.random.key(seed), 4)
    wavefunctions = draw_wavefunctions(jax.random.fold_in(key_of[3], 71), 0)
    potential = draw_potential(jax.random.fold_in(key_of[3], 71), 0)
    occupation = jnp.clip(jnp.exp(math.log(1.0) - 2.9957323 * jax.random.uniform(key_of[2], (BANDS,), jnp.float32) ** shard_levels(key_of[2], (BANDS,), ((0, 2),), -0.2, 0.2)), 0.05, 1.0)
    return dict(wavefunctions=wavefunctions, potential=potential, occupation=occupation)


SPACING = 0.4
TIME_STEP = 0.012
KAPPA_PBE = 0.804
MU_PBE = 0.21951
FERMI_FACTOR = 2.0 * math.pow(3.0 * math.pi * math.pi, 1.0 / 3.0)
SLATER_FACTOR = 0.75 * math.pow(3.0 / math.pi, 1.0 / 3.0)

def kinetic_grid():
    wavenumber = jnp.fft.fftfreq(GRID) * (2.0 * math.pi / SPACING)
    squared = wavenumber * wavenumber
    return 0.5 * (squared[:, None, None] + squared[None, :, None] + squared[None, None, :])

def hamiltonian(field, potential, kinetic):
    return jnp.fft.ifftn(kinetic * jnp.fft.fftn(field)) + potential * field

def periodic_derivative(values, dimension):
    nearer = jnp.roll(values, -1, dimension) - jnp.roll(values, 1, dimension)
    farther = jnp.roll(values, -2, dimension) - jnp.roll(values, 2, dimension)
    return (8.0 * nearer - farther) / (12.0 * SPACING)

def exchange_terms(density, grad_z, grad_x, grad_y):
    gradient_norm = jnp.sqrt(grad_z * grad_z + grad_x * grad_x + grad_y * grad_y)
    power = jnp.power(density, 4.0 / 3.0)
    reduced = gradient_norm / (FERMI_FACTOR * power)
    enhance = 1.0 + KAPPA_PBE - KAPPA_PBE / (1.0 + MU_PBE * reduced * reduced / KAPPA_PBE)
    return (reduced, -SLATER_FACTOR * power * enhance)

def reference(wavefunctions, potential, occupation):
    kinetic = kinetic_grid()

    def one_band(density, inputs):
        real_part, imag_part, weight = inputs
        field = real_part + 1j * imag_part
        first = hamiltonian(field, potential, kinetic)
        second = hamiltonian(first, potential, kinetic)
        result = field - 1j * TIME_STEP * first - 0.5 * TIME_STEP * TIME_STEP * second
        new_real = jnp.real(result)
        new_imag = jnp.imag(result)
        density = density + weight * (new_real * new_real + new_imag * new_imag)
        return (density, (new_real, new_imag))
    start_density = jnp.zeros(potential.shape, jnp.float32)
    density, outputs = lax.scan(one_band, start_density, (wavefunctions[0], wavefunctions[1], occupation))
    propagated = jnp.stack([outputs[0], outputs[1]])
    grad_z = periodic_derivative(density, 0)
    grad_x = periodic_derivative(density, 1)
    grad_y = periodic_derivative(density, 2)
    reduced, energy = exchange_terms(density, grad_z, grad_x, grad_y)
    return (propagated, reduced, energy)
```

```python
import math

import jax
import jax.numpy as jnp
import numpy as np
from jax import lax
from jax.sharding import PartitionSpec as P

SPACING = 0.4
TIME_STEP = 0.012
KAPPA_PBE = 0.804
MU_PBE = 0.21951
FERMI_FACTOR = 2.0 * math.pow(3.0 * math.pi * math.pi, 1.0 / 3.0)
SLATER_FACTOR = 0.75 * math.pow(3.0 / math.pi, 1.0 / 3.0)


def second_derivative_tables(length):
    counter = np.arange(length)
    signed = np.where(counter < length // 2, counter, counter - length)
    squared = 0.5 * (signed * (2.0 * math.pi / (length * SPACING))) ** 2
    phase = (counter[:, None] * counter[None, :]) % length
    wave = np.cos(phase * (2.0 * math.pi / length))
    once = wave @ squared / length
    twice = wave @ (squared * squared) / length
    offset = (counter[:, None] - counter[None, :]) % length
    return (once[offset].astype(np.float32), twice[offset].astype(np.float32))


def along(values, table, formula):
    return jnp.einsum(
        formula,
        values,
        table,
        precision=lax.Precision.HIGHEST,
        preferred_element_type=jnp.float32,
    )


def in_plane(values, table):
    return along(values, table, "kzxy,xe->kzey") + along(values, table, "kzxy,ye->kzxe")


def to_columns(values):
    return lax.all_to_all(values, "fft", split_axis=2, concat_axis=1, tiled=True)


def to_planes(values):
    return lax.all_to_all(values, "fft", split_axis=1, concat_axis=2, tiled=True)


def fourth_order(padded, dimension):
    length = padded.shape[dimension] - 4

    def shifted(offset):
        return lax.slice_in_dim(padded, offset, offset + length, axis=dimension)

    return (8.0 * (shifted(3) - shifted(1)) - (shifted(4) - shifted(0))) / (12.0 * SPACING)


def periodic_derivative(values, dimension):
    nearer = jnp.roll(values, -1, dimension) - jnp.roll(values, 1, dimension)
    farther = jnp.roll(values, -2, dimension) - jnp.roll(values, 2, dimension)
    return (8.0 * nearer - farther) / (12.0 * SPACING)


def exchange_terms(density, grad_z, grad_x, grad_y):
    gradient_norm = jnp.sqrt(grad_z * grad_z + grad_x * grad_x + grad_y * grad_y)
    power = jnp.power(density, 4.0 / 3.0)
    reduced = gradient_norm / (FERMI_FACTOR * power)
    enhance = 1.0 + KAPPA_PBE - KAPPA_PBE / (1.0 + MU_PBE * reduced * reduced / KAPPA_PBE)
    return (reduced, -SLATER_FACTOR * power * enhance)


def padded_density(partial):
    slabs, groups = (lax.axis_size("fft"), lax.axis_size("band"))
    width = partial.shape[1] // groups
    extended = jnp.concatenate([partial[:, -2:], partial, partial[:, :2]], axis=1)
    own = lax.axis_index("band")
    center, before, after = (0.0, 0.0, 0.0)
    for step in range(groups):
        target = lax.rem(own + step, groups)
        window = lax.dynamic_slice_in_dim(extended, target * width, width + 4, axis=1)

        def send(values, shift):
            pairs = [
                (f * groups + b, (f + shift) % slabs * groups + (b + step) % groups)
                for f in range(slabs)
                for b in range(groups)
            ]
            return lax.ppermute(values, ("fft", "band"), pairs)

        before = before + send(window[-2:], 1)
        after = after + send(window[:2], -1)
        center = center + (window if step == 0 else send(window, 0))
    return jnp.concatenate([before, center, after], axis=0)


def per_device(wavefunctions, potential, occupation):
    parts, bands, depth, length, _ = wavefunctions.shape
    once, twice = second_derivative_tables(length)
    field = wavefunctions.reshape(parts * bands, depth, length, length)
    columns = to_columns(jnp.concatenate([field, potential[None]], axis=0))
    local = in_plane(field, once) + potential * field
    field_columns, potential_columns = (columns[:-1], columns[-1:])
    normal_columns = along(field_columns, once, "kzxy,ze->kexy")
    normal = to_planes(normal_columns)
    weighted_columns = normal_columns + potential_columns * field_columns
    normal_second = to_planes(along(weighted_columns, once, "kzxy,ze->kexy"))
    first = normal + local
    second = in_plane(normal + first, once) + potential * first + normal_second
    shape = wavefunctions.shape
    first = first.reshape(shape)
    second = second.reshape(shape)
    result = jnp.stack([
        wavefunctions[0] + TIME_STEP * first[1] - 0.5 * TIME_STEP * TIME_STEP * second[0],
        wavefunctions[1] - TIME_STEP * first[0] - 0.5 * TIME_STEP * TIME_STEP * second[1],
    ])
    squares = result[0] * result[0] + result[1] * result[1]
    padded = padded_density(jnp.sum(occupation[:, None, None, None] * squares, axis=0))
    center = padded[2:-2, 2:-2]
    grad_z = fourth_order(padded[:, 2:-2], 0)
    grad_x = fourth_order(padded[2:-2], 1)
    grad_y = periodic_derivative(center, 2)
    reduced, energy = exchange_terms(center, grad_z, grad_x, grad_y)
    return (result, reduced, energy)


def solution(mesh):
    in_specs = (P(None, "band", "fft", None, None), P("fft", None, None), P("band"))
    out_specs = (P(None, "band", "fft", None, None), P("fft", "band", None), P("fft", "band", None))
    return jax.shard_map(
        per_device, mesh=mesh, in_specs=in_specs, out_specs=out_specs, check_vma=False
    )
```

```python
import functools
import math

import jax
import jax.numpy as jnp
import numpy as np
from jax import lax
from jax.experimental import pallas as pl
from jax.experimental.pallas import tpu as pltpu
from jax.sharding import PartitionSpec as P

SPACING = 0.4
TIME_STEP = 0.012
KAPPA_PBE = 0.804
MU_PBE = 0.21951
FERMI_FACTOR = 2.0 * math.pow(3.0 * math.pi * math.pi, 1.0 / 3.0)
SLATER_FACTOR = 0.75 * math.pow(3.0 / math.pi, 1.0 / 3.0)


def second_derivative(length):
    counter = np.arange(length)
    signed = np.where(counter < length // 2, counter, counter - length)
    squared = 0.5 * (signed * (2.0 * math.pi / (length * SPACING))) ** 2
    phase = (counter[:, None] * counter[None, :]) % length
    wave = np.cos(phase * (2.0 * math.pi / length))
    offset = (counter[:, None] - counter[None, :]) % length
    return (wave @ squared / length)[offset].astype(np.float32)


def along(values, table, formula):
    return jnp.einsum(
        formula,
        values,
        table,
        precision=lax.Precision.HIGHEST,
        preferred_element_type=jnp.float32,
    )


def in_plane(values, table):
    return along(values, table, "kzxy,xe->kzey") + along(values, table, "kzxy,ye->kzxe")


def to_columns(values):
    return lax.all_to_all(values, "fft", split_axis=2, concat_axis=1, tiled=True)


def to_planes(values):
    return lax.all_to_all(values, "fft", split_axis=1, concat_axis=2, tiled=True)


def fourth_order(padded, dimension):
    length = padded.shape[dimension] - 4

    def shifted(offset):
        return lax.slice_in_dim(padded, offset, offset + length, axis=dimension)

    return (8.0 * (shifted(3) - shifted(1)) - (shifted(4) - shifted(0))) / (12.0 * SPACING)


def periodic_derivative(values, dimension):
    nearer = jnp.roll(values, -1, dimension) - jnp.roll(values, 1, dimension)
    farther = jnp.roll(values, -2, dimension) - jnp.roll(values, 2, dimension)
    return (8.0 * nearer - farther) / (12.0 * SPACING)


def exchange_terms(density, grad_z, grad_x, grad_y):
    gradient_norm = jnp.sqrt(grad_z * grad_z + grad_x * grad_x + grad_y * grad_y)
    power = jnp.power(density, 4.0 / 3.0)
    reduced = gradient_norm / (FERMI_FACTOR * power)
    enhance = 1.0 + KAPPA_PBE - KAPPA_PBE / (1.0 + MU_PBE * reduced * reduced / KAPPA_PBE)
    return (reduced, -SLATER_FACTOR * power * enhance)


def padded_density(partial):
    slabs, groups = (lax.axis_size("fft"), lax.axis_size("band"))
    width = partial.shape[1] // groups
    extended = jnp.concatenate([partial[:, -2:], partial, partial[:, :2]], axis=1)
    own = lax.axis_index("band")
    center, before, after = (0.0, 0.0, 0.0)
    for step in range(groups):
        target = lax.rem(own + step, groups)
        window = lax.dynamic_slice_in_dim(extended, target * width, width + 4, axis=1)

        def send(values, shift):
            pairs = [
                (f * groups + b, (f + shift) % slabs * groups + (b + step) % groups)
                for f in range(slabs)
                for b in range(groups)
            ]
            return lax.ppermute(values, ("fft", "band"), pairs)

        before = before + send(window[-2:], 1)
        after = after + send(window[:2], -1)
        center = center + (window if step == 0 else send(window, 0))
    return jnp.concatenate([before, center, after], axis=0)


def step_with_collectives(wavefunctions, potential, occupation):
    parts, bands, depth, length, _ = wavefunctions.shape
    once = second_derivative(length)
    field = wavefunctions.reshape(parts * bands, depth, length, length)
    columns = to_columns(jnp.concatenate([field, potential[None]], axis=0))
    local = in_plane(field, once) + potential * field
    field_columns, potential_columns = (columns[:-1], columns[-1:])
    normal_columns = along(field_columns, once, "kzxy,ze->kexy")
    normal = to_planes(normal_columns)
    weighted_columns = normal_columns + potential_columns * field_columns
    normal_second = to_planes(along(weighted_columns, once, "kzxy,ze->kexy"))
    first = normal + local
    second = in_plane(normal + first, once) + potential * first + normal_second
    shape = wavefunctions.shape
    first = first.reshape(shape)
    second = second.reshape(shape)
    result = jnp.stack([
        wavefunctions[0] + TIME_STEP * first[1] - 0.5 * TIME_STEP * TIME_STEP * second[0],
        wavefunctions[1] - TIME_STEP * first[0] - 0.5 * TIME_STEP * TIME_STEP * second[1],
    ])
    squares = result[0] * result[0] + result[1] * result[1]
    partial = jnp.sum(occupation[:, None, None, None] * squares, axis=0)
    return (result, padded_density(partial))


MESH = pl.DeviceIdType.MESH
EDGE = 8


def multiply(left, right):
    return jnp.dot(
        left,
        right,
        precision=lax.Precision.HIGHEST,
        preferred_element_type=jnp.float32,
    )


def step_kernel(
    slabs, groups, psi, pot, occ, table, out, dens,
    psi_v, pot_v, psi_col, pot_col, normal_col, second_col, normal, second, local,
    result, partial, arrived,
    send_sem, recv_sem, local_sem, dens_send, dens_recv,
):
    parts, bands, depth, length, _ = psi.shape
    rows = length // slabs
    width = length // groups
    me = lax.axis_index("fft")
    own = lax.axis_index("band")
    half = 0.5 * TIME_STEP * TIME_STEP

    barrier = pltpu.get_barrier_semaphore()

    def greet(step, carry):
        peer = lax.rem(me + step, slabs)
        pl.semaphore_signal(barrier, inc=1, device_id={"fft": peer}, device_id_type=MESH)
        return carry

    lax.fori_loop(1, slabs, greet, 0)
    count = slabs - 1
    for group in range(1, groups):
        for shift in (0, 1, slabs - 1):
            there = {"fft": lax.rem(me + shift, slabs), "band": lax.rem(own + group, groups)}
            pl.semaphore_signal(barrier, inc=1, device_id=there, device_id_type=MESH)
            count += 1

    load_psi = pltpu.make_async_copy(psi, psi_v, local_sem.at[0])
    load_pot = pltpu.make_async_copy(pot, pot_v, local_sem.at[1])
    load_psi.start()
    load_pot.start()
    pl.semaphore_wait(barrier, count)

    def x_rows(device):
        return pl.ds(pl.multiple_of(device * rows, rows), rows)

    def z_planes(device):
        return pl.ds(pl.multiple_of(device * depth, depth), depth)

    def ends(chunk, device):
        if chunk < bands:
            return (psi.at[:, chunk, :, x_rows(device)], psi_col.at[chunk, :, z_planes(me)])
        if chunk == bands:
            return (pot.at[:, x_rows(device)], pot_col.at[z_planes(me)])
        if chunk <= 2 * bands:
            band = chunk - bands - 1
            return (normal_col.at[band, :, z_planes(device)], normal.at[band, :, :, x_rows(me)])
        band = chunk - 2 * bands - 1
        return (second_col.at[band, :, z_planes(device)], second.at[band, :, :, x_rows(me)])

    def remote(chunk, device, slot):
        source, target = ends(chunk, device)
        return pltpu.make_async_remote_copy(
            src_ref=source,
            dst_ref=target,
            send_sem=send_sem.at[chunk, device],
            recv_sem=recv_sem.at[chunk, slot],
            device_id={"fft": device},
            device_id_type=MESH,
        )

    def keep(chunk):
        source, target = ends(chunk, me)
        return pltpu.make_async_copy(source, target, local_sem.at[2 + chunk])

    def post(chunk):
        def one(step, carry):
            remote(chunk, lax.rem(me + step, slabs), me).start()
            return carry

        lax.fori_loop(1, slabs, one, 0)
        keep(chunk).start()

    def collect(chunk):
        def one(step, carry):
            device = lax.rem(me + slabs - step, slabs)
            remote(chunk, device, device).wait_recv()
            return carry

        lax.fori_loop(1, slabs, one, 0)
        keep(chunk).wait()

    for chunk in range(bands + 1):
        post(chunk)

    matrix = table[...]
    load_psi.wait()
    load_pot.wait()

    def in_planes(index, carry):
        part = index // (bands * depth)
        band = index // depth % bands
        z = index % depth
        values = psi_v[part, band, z]
        local[band, part, z] = (
            multiply(matrix, values) + multiply(values, matrix) + pot_v[z] * values
        )
        return carry

    lax.fori_loop(0, parts * bands * depth, in_planes, 0)

    def strided(ref, row):
        return (ref.reshape(length * rows, length), pl.ds(row, length, stride=rows))

    def load(ref, row):
        flat, span = strided(ref, row)
        return flat[span, :]

    def store(ref, row, values):
        flat, span = strided(ref, row)
        flat[span, :] = values

    for band in range(bands):
        collect(band)
        for part in range(parts):
            for row in range(rows):
                values = load(psi_col.at[band, part], row)
                store(normal_col.at[band, part], row, multiply(matrix, values))
        post(bands + 1 + band)
    collect(bands)
    for band in range(bands):
        for part in range(parts):
            for row in range(rows):
                values = load(normal_col.at[band, part], row)
                values += load(pot_col, row) * load(psi_col.at[band, part], row)
                store(second_col.at[band, part], row, multiply(matrix, values))
        post(2 * bands + 1 + band)

    for band in range(bands):
        collect(bands + 1 + band)

        def advance(z, carry):
            firsts = []
            seconds = []
            for part in range(parts):
                kinetic = normal[band, part, z]
                first = kinetic + local[band, part, z]
                both = kinetic + first
                firsts.append(first)
                seconds.append(
                    multiply(matrix, both) + multiply(both, matrix) + pot_v[z] * first
                )
            result[0, band, z] = psi_v[0, band, z] + TIME_STEP * firsts[1] - half * seconds[0]
            result[1, band, z] = psi_v[1, band, z] - TIME_STEP * firsts[0] - half * seconds[1]
            return carry

        lax.fori_loop(0, depth, advance, 0)

    for band in range(bands):
        collect(2 * bands + 1 + band)
        weight = occ[band]

        def finish(z, carry):
            real = result[0, band, z] - half * second[band, 0, z]
            imag = result[1, band, z] - half * second[band, 1, z]
            result[0, band, z] = real
            result[1, band, z] = imag
            share = weight * (real * real + imag * imag)
            partial[z] = share if band == 0 else partial[z] + share
            return carry

        lax.fori_loop(0, depth, finish, 0)

    def window_copies(group):
        target = lax.rem(own + group, groups)
        spans = (
            (lax.rem(target * width + length - EDGE, length), 0, EDGE),
            (target * width, EDGE, width),
            (lax.rem(target * width + width, length), EDGE + width, EDGE),
        )
        found = []
        for shift, z_from, z_to, planes in (
            (1, depth - 2, 0, 2), (slabs - 1, 0, depth + 2, 2), (0, 0, 2, depth),
        ):
            if shift == 0 and group == 0:
                continue
            there = {"fft": lax.rem(me + shift, slabs), "band": target}
            for x_from, x_to, size in spans:
                slot = len(found)
                found.append(pltpu.make_async_remote_copy(
                    src_ref=partial.at[pl.ds(z_from, planes), pl.ds(pl.multiple_of(x_from, EDGE), size)],
                    dst_ref=arrived.at[group, pl.ds(z_to, planes), pl.ds(x_to, size)],
                    send_sem=dens_send.at[group, slot],
                    recv_sem=dens_recv.at[group, slot],
                    device_id=there,
                    device_id_type=MESH,
                ))
        return found

    exchange = [copy for group in reversed(range(groups)) for copy in window_copies(group)]
    for copy in exchange:
        copy.start()
    write = pltpu.make_async_copy(result, out, local_sem.at[0])
    write.start()
    keep_window = []
    for slot, (x_from, x_to, size) in enumerate((
        (lax.rem(own * width + length - EDGE, length), 0, EDGE),
        (own * width, EDGE, width),
        (lax.rem(own * width + width, length), EDGE + width, EDGE),
    )):
        copy = pltpu.make_async_copy(
            partial.at[:, pl.ds(pl.multiple_of(x_from, EDGE), size)],
            arrived.at[0, pl.ds(2, depth), pl.ds(x_to, size)],
            dens_send.at[groups, slot],
        )
        copy.start()
        keep_window.append(copy)

    for chunk in range(3 * bands + 1):
        def drain(step, carry):
            remote(chunk, lax.rem(me + step, slabs), me).wait_send()
            return carry

        lax.fori_loop(1, slabs, drain, 0)
    for copy in keep_window:
        copy.wait()
    for copy in exchange:
        copy.wait_recv()

    def total(z, carry):
        value = arrived[0, z]
        for group in range(1, groups):
            value += arrived[group, z]
        dens[z] = value
        return carry

    lax.fori_loop(0, depth + 4, total, 0)
    for copy in exchange:
        copy.wait_send()
    write.wait()


def step_in_kernel(wavefunctions, potential, occupation):
    parts, bands, depth, length, _ = wavefunctions.shape
    slabs, groups = (lax.axis_size("fft"), lax.axis_size("band"))
    rows, width = (length // slabs, length // groups)
    table = jnp.asarray(second_derivative(length))
    chunks = 3 * bands + 1
    by_band = pltpu.VMEM((bands, parts, depth, length, length), jnp.float32)
    by_part = pltpu.VMEM((parts, bands, depth, length, length), jnp.float32)
    columns = pltpu.VMEM((bands, parts, length, rows, length), jnp.float32)
    plane = (width + 2 * EDGE, length)
    result, padded = pl.pallas_call(
        functools.partial(step_kernel, slabs, groups),
        out_shape=(
            jax.ShapeDtypeStruct(wavefunctions.shape, jnp.float32),
            jax.ShapeDtypeStruct((depth + 4,) + plane, jnp.float32),
        ),
        in_specs=[
            pl.BlockSpec(memory_space=pl.ANY),
            pl.BlockSpec(memory_space=pl.ANY),
            pl.BlockSpec(memory_space=pltpu.SMEM),
            pl.BlockSpec(memory_space=pltpu.VMEM),
        ],
        out_specs=(
            pl.BlockSpec(memory_space=pl.ANY),
            pl.BlockSpec(memory_space=pltpu.VMEM),
        ),
        scratch_shapes=[
            by_part,
            pltpu.VMEM((depth, length, length), jnp.float32),
            columns,
            pltpu.VMEM((length, rows, length), jnp.float32),
            columns,
            columns,
            by_band,
            by_band,
            by_band,
            by_part,
            pltpu.VMEM((depth, length, length), jnp.float32),
            pltpu.VMEM((groups, depth + 4) + plane, jnp.float32),
            pltpu.SemaphoreType.DMA((chunks, slabs)),
            pltpu.SemaphoreType.DMA((chunks, slabs)),
            pltpu.SemaphoreType.DMA((chunks + 2,)),
            pltpu.SemaphoreType.DMA((groups + 1, 9)),
            pltpu.SemaphoreType.DMA((groups, 9)),
        ],
        compiler_params=pltpu.CompilerParams(
            collective_id=0, has_side_effects=True, vmem_limit_bytes=48 * 1024 * 1024
        ),
    )(wavefunctions, potential, occupation, table)
    return (result, padded[:, EDGE - 2 : EDGE + width + 2])


def per_device(wavefunctions, potential, occupation):
    _, _, depth, length, _ = wavefunctions.shape
    rows = length // lax.axis_size("fft")
    whole_tiles = rows % 8 == 0 and depth % 8 == 0 and lax.axis_size("band") == 2
    step = step_in_kernel if whole_tiles else step_with_collectives
    result, padded = step(wavefunctions, potential, occupation)
    center = padded[2:-2, 2:-2]
    grad_z = fourth_order(padded[:, 2:-2], 0)
    grad_x = fourth_order(padded[2:-2], 1)
    grad_y = periodic_derivative(center, 2)
    reduced, energy = exchange_terms(center, grad_z, grad_x, grad_y)
    return (result, reduced, energy)


def solution(mesh):
    in_specs = (P(None, "band", "fft", None, None), P("fft", None, None), P("band"))
    out_specs = (P(None, "band", "fft", None, None), P("fft", "band", None), P("fft", "band", None))
    return jax.shard_map(
        per_device, mesh=mesh, in_specs=in_specs, out_specs=out_specs, check_vma=False
    )
```

```python
import functools
import math

import jax
import jax.numpy as jnp
import numpy as np
from jax import lax
from jax.experimental import pallas as pl
from jax.experimental.pallas import tpu as pltpu
from jax.sharding import PartitionSpec as P

SPACING = 0.4
TIME_STEP = 0.012
KAPPA_PBE = 0.804
MU_PBE = 0.21951
FERMI_FACTOR = 2.0 * math.pow(3.0 * math.pi * math.pi, 1.0 / 3.0)
SLATER_FACTOR = 0.75 * math.pow(3.0 / math.pi, 1.0 / 3.0)


def second_derivative(length):
    counter = np.arange(length)
    signed = np.where(counter < length // 2, counter, counter - length)
    squared = 0.5 * (signed * (2.0 * math.pi / (length * SPACING))) ** 2
    phase = (counter[:, None] * counter[None, :]) % length
    wave = np.cos(phase * (2.0 * math.pi / length))
    offset = (counter[:, None] - counter[None, :]) % length
    return (wave @ squared / length)[offset].astype(np.float32)


def along(values, table, formula):
    return jnp.einsum(
        formula,
        values,
        table,
        precision=lax.Precision.HIGHEST,
        preferred_element_type=jnp.float32,
    )


def in_plane(values, table):
    return along(values, table, "kzxy,xe->kzey") + along(values, table, "kzxy,ye->kzxe")


def to_columns(values):
    return lax.all_to_all(values, "fft", split_axis=2, concat_axis=1, tiled=True)


def to_planes(values):
    return lax.all_to_all(values, "fft", split_axis=1, concat_axis=2, tiled=True)


def fourth_order(padded, dimension):
    length = padded.shape[dimension] - 4

    def shifted(offset):
        return lax.slice_in_dim(padded, offset, offset + length, axis=dimension)

    return (8.0 * (shifted(3) - shifted(1)) - (shifted(4) - shifted(0))) / (12.0 * SPACING)


def periodic_derivative(values, dimension):
    nearer = jnp.roll(values, -1, dimension) - jnp.roll(values, 1, dimension)
    farther = jnp.roll(values, -2, dimension) - jnp.roll(values, 2, dimension)
    return (8.0 * nearer - farther) / (12.0 * SPACING)


def exchange_terms(density, grad_z, grad_x, grad_y):
    gradient_norm = jnp.sqrt(grad_z * grad_z + grad_x * grad_x + grad_y * grad_y)
    power = jnp.power(density, 4.0 / 3.0)
    reduced = gradient_norm / (FERMI_FACTOR * power)
    enhance = 1.0 + KAPPA_PBE - KAPPA_PBE / (1.0 + MU_PBE * reduced * reduced / KAPPA_PBE)
    return (reduced, -SLATER_FACTOR * power * enhance)


def padded_density(partial):
    slabs, groups = (lax.axis_size("fft"), lax.axis_size("band"))
    width = partial.shape[1] // groups
    extended = jnp.concatenate([partial[:, -2:], partial, partial[:, :2]], axis=1)
    own = lax.axis_index("band")
    center, before, after = (0.0, 0.0, 0.0)
    for step in range(groups):
        target = lax.rem(own + step, groups)
        window = lax.dynamic_slice_in_dim(extended, target * width, width + 4, axis=1)

        def send(values, shift):
            pairs = [
                (f * groups + b, (f + shift) % slabs * groups + (b + step) % groups)
                for f in range(slabs)
                for b in range(groups)
            ]
            return lax.ppermute(values, ("fft", "band"), pairs)

        before = before + send(window[-2:], 1)
        after = after + send(window[:2], -1)
        center = center + (window if step == 0 else send(window, 0))
    return jnp.concatenate([before, center, after], axis=0)


def step_with_collectives(wavefunctions, potential, occupation):
    parts, bands, depth, length, _ = wavefunctions.shape
    once = second_derivative(length)
    field = wavefunctions.reshape(parts * bands, depth, length, length)
    columns = to_columns(jnp.concatenate([field, potential[None]], axis=0))
    local = in_plane(field, once) + potential * field
    field_columns, potential_columns = (columns[:-1], columns[-1:])
    normal_columns = along(field_columns, once, "kzxy,ze->kexy")
    normal = to_planes(normal_columns)
    weighted_columns = normal_columns + potential_columns * field_columns
    normal_second = to_planes(along(weighted_columns, once, "kzxy,ze->kexy"))
    first = normal + local
    second = in_plane(normal + first, once) + potential * first + normal_second
    shape = wavefunctions.shape
    first = first.reshape(shape)
    second = second.reshape(shape)
    result = jnp.stack([
        wavefunctions[0] + TIME_STEP * first[1] - 0.5 * TIME_STEP * TIME_STEP * second[0],
        wavefunctions[1] - TIME_STEP * first[0] - 0.5 * TIME_STEP * TIME_STEP * second[1],
    ])
    squares = result[0] * result[0] + result[1] * result[1]
    partial = jnp.sum(occupation[:, None, None, None] * squares, axis=0)
    return (result, padded_density(partial))


MESH = pl.DeviceIdType.MESH
EDGE = 8


def multiply(left, right):
    return jnp.dot(
        left,
        right,
        precision=lax.Precision.HIGHEST,
        preferred_element_type=jnp.float32,
    )


def step_kernel(
    slabs, groups, psi, pot, occ, table, out, dens,
    psi_v, pot_v, psi_col, pot_col, normal_col, second_col, normal, second, local,
    result, partial, arrived,
    send_sem, recv_sem, local_sem, dens_send, dens_recv, pot_send, pot_recv,
):
    parts, bands, depth, length, _ = psi.shape
    fields = bands * parts
    members = slabs // 2
    rows = length // members
    share_rows = rows // groups
    width = length // groups
    me = lax.axis_index("fft")
    own = lax.axis_index("band")
    place = lax.rem(me, members)
    base = me - place
    half = 0.5 * TIME_STEP * TIME_STEP

    barrier = pltpu.get_barrier_semaphore()

    def greet(step, carry):
        peer = lax.rem(me + step, slabs)
        pl.semaphore_signal(barrier, inc=1, device_id={"fft": peer}, device_id_type=MESH)
        return carry

    lax.fori_loop(1, slabs, greet, 0)
    count = slabs - 1
    for group in range(1, groups):
        for shift in (0, 1, slabs - 1):
            there = {"fft": lax.rem(me + shift, slabs), "band": lax.rem(own + group, groups)}
            pl.semaphore_signal(barrier, inc=1, device_id=there, device_id_type=MESH)
            count += 1

    load_psi = pltpu.make_async_copy(psi, psi_v, local_sem.at[0])
    load_pot = pltpu.make_async_copy(pot, pot_v, local_sem.at[1])
    load_psi.start()
    load_pot.start()
    pl.semaphore_wait(barrier, count)

    def x_rows(device):
        return pl.ds(pl.multiple_of(lax.rem(device, members) * rows, rows), rows)

    def z_planes(device):
        return pl.ds(pl.multiple_of(device * depth, depth), depth)

    def half_planes(device):
        return pl.ds(pl.multiple_of(lax.rem(device, members) * depth, depth), depth)

    def shared(start, group):
        first = start + group * share_rows
        return pl.ds(pl.multiple_of(first, share_rows), share_rows)

    def ends(chunk, device):
        if chunk == fields:
            start = lax.rem(device, members) * rows
            return (pot.at[:, shared(start, own)], pot_col.at[z_planes(me), shared(0, own)])
        kind, field = divmod(chunk - (chunk > fields), fields)
        band, part = divmod(field, parts)
        if kind == 0:
            return (psi.at[part, band, :, x_rows(device)], psi_col.at[band, part, z_planes(me)])
        if kind == 1:
            return (
                normal_col.at[band, part, z_planes(device)],
                normal.at[band, part, :, x_rows(me)],
            )
        return (
            second_col.at[band, part, half_planes(device)],
            second.at[band, part, :, x_rows(me)],
        )

    def partners(chunk):
        return slabs if chunk <= fields else members

    def partner(chunk, step):
        if chunk <= fields:
            return lax.rem(me + step, slabs)
        return base + lax.rem(place + step, members)

    def remote(chunk, device, slot):
        source, target = ends(chunk, device)
        return pltpu.make_async_remote_copy(
            src_ref=source,
            dst_ref=target,
            send_sem=send_sem.at[chunk, device],
            recv_sem=recv_sem.at[chunk, slot],
            device_id={"fft": device},
            device_id_type=MESH,
        )

    def keep(chunk):
        source, target = ends(chunk, me)
        return pltpu.make_async_copy(source, target, local_sem.at[2 + chunk])

    def post(chunk):
        def one(step, carry):
            remote(chunk, partner(chunk, step), me).start()
            return carry

        lax.fori_loop(1, partners(chunk), one, 0)
        keep(chunk).start()

    def collect(chunk):
        def one(step, carry):
            device = partner(chunk, partners(chunk) - step)
            remote(chunk, device, device).wait_recv()
            return carry

        lax.fori_loop(1, partners(chunk), one, 0)
        keep(chunk).wait()

    post(0)
    post(fields)
    post(1)

    matrix = table[...]
    half_matrix = table[pl.ds(pl.multiple_of(base * depth, members * depth), members * depth), :]
    load_psi.wait()
    load_pot.wait()

    def in_planes(index, carry):
        part = index // (bands * depth)
        band = index // depth % bands
        z = index % depth
        values = psi_v[part, band, z]
        local[band, part, z] = (
            multiply(matrix, values) + multiply(values, matrix) + pot_v[z] * values
        )
        return carry

    lax.fori_loop(0, parts * bands * depth, in_planes, 0)

    def load(ref, row):
        return ref.reshape(length * rows, length)[pl.ds(row, length, stride=rows), :]

    def store(ref, row, planes, values):
        ref.reshape(planes * rows, length)[pl.ds(row, planes, stride=rows), :] = values

    def once(field):
        band, part = divmod(field, parts)
        collect(field)
        for row in range(rows):
            values = load(psi_col.at[band, part], row)
            store(normal_col.at[band, part], row, length, multiply(matrix, values))
        post(fields + 1 + field)

    def twice(field):
        band, part = divmod(field, parts)
        planes = members * depth
        for row in range(rows):
            values = load(normal_col.at[band, part], row)
            values += load(pot_col, row) * load(psi_col.at[band, part], row)
            store(second_col.at[band, part], row, planes, multiply(half_matrix, values))
        post(2 * fields + 1 + field)

    def pot_copy(group, source):
        return pltpu.make_async_remote_copy(
            src_ref=pot_col.at[:, shared(0, source)],
            dst_ref=pot_col.at[:, shared(0, source)],
            send_sem=pot_send.at[group],
            recv_sem=pot_recv.at[group],
            device_id={"band": lax.rem(own + group, groups)},
            device_id_type=MESH,
        )

    def first_part(band):
        for part in range(parts):
            collect(fields + 1 + band * parts + part)

        def advance(z, carry):
            firsts = []
            seconds = []
            for part in range(parts):
                kinetic = normal[band, part, z]
                first = kinetic + local[band, part, z]
                both = kinetic + first
                firsts.append(first)
                seconds.append(
                    multiply(matrix, both) + multiply(both, matrix) + pot_v[z] * first
                )
            result[0, band, z] = psi_v[0, band, z] + TIME_STEP * firsts[1] - half * seconds[0]
            result[1, band, z] = psi_v[1, band, z] - TIME_STEP * firsts[0] - half * seconds[1]
            return carry

        lax.fori_loop(0, depth, advance, 0)

    def last_part(band):
        for part in range(parts):
            collect(2 * fields + 1 + band * parts + part)
        weight = occ[band]

        def finish(z, carry):
            real = result[0, band, z] - half * second[band, 0, z]
            imag = result[1, band, z] - half * second[band, 1, z]
            result[0, band, z] = real
            result[1, band, z] = imag
            share = weight * (real * real + imag * imag)
            partial[z] = share if band == 0 else partial[z] + share
            return carry

        lax.fori_loop(0, depth, finish, 0)

    once(0)
    post(2)
    collect(fields)
    for group in range(1, groups):
        pot_copy(group, own).start()
    once(1)
    for field in range(3, fields):
        post(field)
    for group in range(1, groups):
        pot_copy(group, lax.rem(own + groups - group, groups)).wait_recv()
    twice(0)
    twice(1)
    for field in range(2, fields - 1):
        once(field)
        twice(field)
    first_part(0)
    once(fields - 1)
    twice(fields - 1)
    last_part(0)
    for band in range(1, bands):
        first_part(band)
        last_part(band)

    def window_copies(group):
        target = lax.rem(own + group, groups)
        spans = (
            (lax.rem(target * width + length - EDGE, length), 0, EDGE),
            (target * width, EDGE, width),
            (lax.rem(target * width + width, length), EDGE + width, EDGE),
        )
        found = []
        for shift, z_from, z_to, planes in (
            (1, depth - 2, 0, 2), (slabs - 1, 0, depth + 2, 2), (0, 0, 2, depth),
        ):
            if shift == 0 and group == 0:
                continue
            there = {"fft": lax.rem(me + shift, slabs), "band": target}
            for x_from, x_to, size in spans:
                slot = len(found)
                found.append(pltpu.make_async_remote_copy(
                    src_ref=partial.at[pl.ds(z_from, planes), pl.ds(pl.multiple_of(x_from, EDGE), size)],
                    dst_ref=arrived.at[group, pl.ds(z_to, planes), pl.ds(x_to, size)],
                    send_sem=dens_send.at[group, slot],
                    recv_sem=dens_recv.at[group, slot],
                    device_id=there,
                    device_id_type=MESH,
                ))
        return found

    exchange = [copy for group in reversed(range(groups)) for copy in window_copies(group)]
    for copy in exchange:
        copy.start()
    write = pltpu.make_async_copy(result, out, local_sem.at[0])
    write.start()
    keep_window = []
    for slot, (x_from, x_to, size) in enumerate((
        (lax.rem(own * width + length - EDGE, length), 0, EDGE),
        (own * width, EDGE, width),
        (lax.rem(own * width + width, length), EDGE + width, EDGE),
    )):
        copy = pltpu.make_async_copy(
            partial.at[:, pl.ds(pl.multiple_of(x_from, EDGE), size)],
            arrived.at[0, pl.ds(2, depth), pl.ds(x_to, size)],
            dens_send.at[groups, slot],
        )
        copy.start()
        keep_window.append(copy)

    for chunk in range(3 * fields + 1):
        def drain(step, carry):
            remote(chunk, partner(chunk, step), me).wait_send()
            return carry

        lax.fori_loop(1, partners(chunk), drain, 0)
    for group in range(1, groups):
        pot_copy(group, own).wait_send()
    for copy in keep_window:
        copy.wait()
    for copy in exchange:
        copy.wait_recv()

    def total(z, carry):
        value = arrived[0, z]
        for group in range(1, groups):
            value += arrived[group, z]
        dens[z] = value
        return carry

    lax.fori_loop(0, depth + 4, total, 0)
    for copy in exchange:
        copy.wait_send()
    write.wait()


def step_in_kernel(wavefunctions, potential, occupation):
    parts, bands, depth, length, _ = wavefunctions.shape
    slabs, groups = (lax.axis_size("fft"), lax.axis_size("band"))
    rows, width = (2 * length // slabs, length // groups)
    table = jnp.asarray(second_derivative(length))
    chunks = 3 * bands * parts + 1
    by_band = pltpu.VMEM((bands, parts, depth, length, length), jnp.float32)
    by_part = pltpu.VMEM((parts, bands, depth, length, length), jnp.float32)
    columns = pltpu.VMEM((bands, parts, length, rows, length), jnp.float32)
    plane = (width + 2 * EDGE, length)
    result, padded = pl.pallas_call(
        functools.partial(step_kernel, slabs, groups),
        out_shape=(
            jax.ShapeDtypeStruct(wavefunctions.shape, jnp.float32),
            jax.ShapeDtypeStruct((depth + 4,) + plane, jnp.float32),
        ),
        in_specs=[
            pl.BlockSpec(memory_space=pl.ANY),
            pl.BlockSpec(memory_space=pl.ANY),
            pl.BlockSpec(memory_space=pltpu.SMEM),
            pl.BlockSpec(memory_space=pltpu.VMEM),
        ],
        out_specs=(
            pl.BlockSpec(memory_space=pl.ANY),
            pl.BlockSpec(memory_space=pltpu.VMEM),
        ),
        scratch_shapes=[
            by_part,
            pltpu.VMEM((depth, length, length), jnp.float32),
            columns,
            pltpu.VMEM((length, rows, length), jnp.float32),
            columns,
            pltpu.VMEM((bands, parts, length // 2, rows, length), jnp.float32),
            by_band,
            by_band,
            by_band,
            by_part,
            pltpu.VMEM((depth, length, length), jnp.float32),
            pltpu.VMEM((groups, depth + 4) + plane, jnp.float32),
            pltpu.SemaphoreType.DMA((chunks, slabs)),
            pltpu.SemaphoreType.DMA((chunks, slabs)),
            pltpu.SemaphoreType.DMA((chunks + 2,)),
            pltpu.SemaphoreType.DMA((groups + 1, 9)),
            pltpu.SemaphoreType.DMA((groups, 9)),
            pltpu.SemaphoreType.DMA((groups,)),
            pltpu.SemaphoreType.DMA((groups,)),
        ],
        compiler_params=pltpu.CompilerParams(
            collective_id=0, has_side_effects=True, vmem_limit_bytes=60 * 1024 * 1024
        ),
    )(wavefunctions, potential, occupation, table)
    return (result, padded[:, EDGE - 2 : EDGE + width + 2])


def per_device(wavefunctions, potential, occupation):
    _, _, depth, length, _ = wavefunctions.shape
    slabs, groups = (lax.axis_size("fft"), lax.axis_size("band"))
    share_rows = 2 * length // slabs // groups
    whole_tiles = slabs % 2 == 0 and groups == 2 and share_rows % 8 == 0
    step = step_in_kernel if whole_tiles else step_with_collectives
    result, padded = step(wavefunctions, potential, occupation)
    center = padded[2:-2, 2:-2]
    grad_z = fourth_order(padded[:, 2:-2], 0)
    grad_x = fourth_order(padded[2:-2], 1)
    grad_y = periodic_derivative(center, 2)
    reduced, energy = exchange_terms(center, grad_z, grad_x, grad_y)
    return (result, reduced, energy)


def solution(mesh):
    in_specs = (P(None, "band", "fft", None, None), P("fft", None, None), P("band"))
    out_specs = (P(None, "band", "fft", None, None), P("fft", "band", None), P("fft", "band", None))
    return jax.shard_map(
        per_device, mesh=mesh, in_specs=in_specs, out_specs=out_specs, check_vma=False
    )
```

```python
import functools
import math

import jax
import jax.numpy as jnp
import numpy as np
from jax import lax
from jax.experimental import pallas as pl
from jax.experimental.pallas import tpu as pltpu
from jax.sharding import PartitionSpec as P

SPACING = 0.4
TIME_STEP = 0.012
KAPPA_PBE = 0.804
MU_PBE = 0.21951
FERMI_FACTOR = 2.0 * math.pow(3.0 * math.pi * math.pi, 1.0 / 3.0)
SLATER_FACTOR = 0.75 * math.pow(3.0 / math.pi, 1.0 / 3.0)


def second_derivative(length):
    counter = np.arange(length)
    signed = np.where(counter < length // 2, counter, counter - length)
    squared = 0.5 * (signed * (2.0 * math.pi / (length * SPACING))) ** 2
    phase = (counter[:, None] * counter[None, :]) % length
    wave = np.cos(phase * (2.0 * math.pi / length))
    offset = (counter[:, None] - counter[None, :]) % length
    return (wave @ squared / length)[offset].astype(np.float32)


def along(values, table, formula):
    return jnp.einsum(
        formula,
        values,
        table,
        precision=lax.Precision.HIGHEST,
        preferred_element_type=jnp.float32,
    )


def in_plane(values, table):
    return along(values, table, "kzxy,xe->kzey") + along(values, table, "kzxy,ye->kzxe")


def to_columns(values):
    return lax.all_to_all(values, "fft", split_axis=2, concat_axis=1, tiled=True)


def to_planes(values):
    return lax.all_to_all(values, "fft", split_axis=1, concat_axis=2, tiled=True)


def fourth_order(padded, dimension):
    length = padded.shape[dimension] - 4

    def shifted(offset):
        return lax.slice_in_dim(padded, offset, offset + length, axis=dimension)

    return (8.0 * (shifted(3) - shifted(1)) - (shifted(4) - shifted(0))) / (12.0 * SPACING)


def periodic_derivative(values, dimension):
    nearer = jnp.roll(values, -1, dimension) - jnp.roll(values, 1, dimension)
    farther = jnp.roll(values, -2, dimension) - jnp.roll(values, 2, dimension)
    return (8.0 * nearer - farther) / (12.0 * SPACING)


def exchange_terms(density, grad_z, grad_x, grad_y):
    gradient_norm = jnp.sqrt(grad_z * grad_z + grad_x * grad_x + grad_y * grad_y)
    power = jnp.power(density, 4.0 / 3.0)
    reduced = gradient_norm / (FERMI_FACTOR * power)
    enhance = 1.0 + KAPPA_PBE - KAPPA_PBE / (1.0 + MU_PBE * reduced * reduced / KAPPA_PBE)
    return (reduced, -SLATER_FACTOR * power * enhance)


def padded_density(partial):
    slabs, groups = (lax.axis_size("fft"), lax.axis_size("band"))
    width = partial.shape[1] // groups
    extended = jnp.concatenate([partial[:, -2:], partial, partial[:, :2]], axis=1)
    own = lax.axis_index("band")
    center, before, after = (0.0, 0.0, 0.0)
    for step in range(groups):
        target = lax.rem(own + step, groups)
        window = lax.dynamic_slice_in_dim(extended, target * width, width + 4, axis=1)

        def send(values, shift):
            pairs = [
                (f * groups + b, (f + shift) % slabs * groups + (b + step) % groups)
                for f in range(slabs)
                for b in range(groups)
            ]
            return lax.ppermute(values, ("fft", "band"), pairs)

        before = before + send(window[-2:], 1)
        after = after + send(window[:2], -1)
        center = center + (window if step == 0 else send(window, 0))
    return jnp.concatenate([before, center, after], axis=0)


def step_with_collectives(wavefunctions, potential, occupation):
    parts, bands, depth, length, _ = wavefunctions.shape
    once = second_derivative(length)
    field = wavefunctions.reshape(parts * bands, depth, length, length)
    columns = to_columns(jnp.concatenate([field, potential[None]], axis=0))
    local = in_plane(field, once) + potential * field
    field_columns, potential_columns = (columns[:-1], columns[-1:])
    normal_columns = along(field_columns, once, "kzxy,ze->kexy")
    normal = to_planes(normal_columns)
    weighted_columns = normal_columns + potential_columns * field_columns
    normal_second = to_planes(along(weighted_columns, once, "kzxy,ze->kexy"))
    first = normal + local
    second = in_plane(normal + first, once) + potential * first + normal_second
    shape = wavefunctions.shape
    first = first.reshape(shape)
    second = second.reshape(shape)
    result = jnp.stack([
        wavefunctions[0] + TIME_STEP * first[1] - 0.5 * TIME_STEP * TIME_STEP * second[0],
        wavefunctions[1] - TIME_STEP * first[0] - 0.5 * TIME_STEP * TIME_STEP * second[1],
    ])
    squares = result[0] * result[0] + result[1] * result[1]
    partial = jnp.sum(occupation[:, None, None, None] * squares, axis=0)
    return (result, padded_density(partial))


MESH = pl.DeviceIdType.MESH
EDGE = 8


def multiply(left, right):
    return jnp.dot(
        left,
        right,
        precision=lax.Precision.HIGH,
        preferred_element_type=jnp.float32,
    )


def step_kernel(
    slabs, groups, psi, pot, occ, table, out, dens,
    psi_v, pot_v, psi_col, pot_col, normal_col, second_col, normal, second, local,
    result, partial, arrived,
    send_sem, recv_sem, local_sem, dens_send, dens_recv, pot_send, pot_recv,
):
    parts, bands, depth, length, _ = psi.shape
    fields = bands * parts
    members = slabs // 2
    rows = length // members
    share_rows = rows // groups
    width = length // groups
    me = lax.axis_index("fft")
    own = lax.axis_index("band")
    place = lax.rem(me, members)
    base = me - place
    half = 0.5 * TIME_STEP * TIME_STEP

    barrier = pltpu.get_barrier_semaphore()

    def greet(step, carry):
        peer = lax.rem(me + step, slabs)
        pl.semaphore_signal(barrier, inc=1, device_id={"fft": peer}, device_id_type=MESH)
        return carry

    lax.fori_loop(1, slabs, greet, 0)
    count = slabs - 1
    for group in range(1, groups):
        for shift in (0, 1, slabs - 1):
            there = {"fft": lax.rem(me + shift, slabs), "band": lax.rem(own + group, groups)}
            pl.semaphore_signal(barrier, inc=1, device_id=there, device_id_type=MESH)
            count += 1

    load_psi = pltpu.make_async_copy(psi, psi_v, local_sem.at[0])
    load_pot = pltpu.make_async_copy(pot, pot_v, local_sem.at[1])
    load_psi.start()
    load_pot.start()
    pl.semaphore_wait(barrier, count)

    def x_rows(device):
        return pl.ds(pl.multiple_of(lax.rem(device, members) * rows, rows), rows)

    def z_planes(device):
        return pl.ds(pl.multiple_of(device * depth, depth), depth)

    def half_planes(device):
        return pl.ds(pl.multiple_of(lax.rem(device, members) * depth, depth), depth)

    def shared(start, group):
        first = start + group * share_rows
        return pl.ds(pl.multiple_of(first, share_rows), share_rows)

    def ends(chunk, device):
        if chunk == fields:
            start = lax.rem(device, members) * rows
            return (pot.at[:, shared(start, own)], pot_col.at[z_planes(me), shared(0, own)])
        kind, field = divmod(chunk - (chunk > fields), fields)
        band, part = divmod(field, parts)
        if kind == 0:
            return (psi.at[part, band, :, x_rows(device)], psi_col.at[band, part, z_planes(me)])
        if kind == 1:
            return (
                normal_col.at[band, part, z_planes(device)],
                normal.at[band, part, :, x_rows(me)],
            )
        return (
            second_col.at[band, part, half_planes(device)],
            second.at[band, part, :, x_rows(me)],
        )

    def partners(chunk):
        return slabs if chunk <= fields else members

    def partner(chunk, step):
        if chunk <= fields:
            return lax.rem(me + step, slabs)
        return base + lax.rem(place + step, members)

    def remote(chunk, device, slot):
        source, target = ends(chunk, device)
        return pltpu.make_async_remote_copy(
            src_ref=source,
            dst_ref=target,
            send_sem=send_sem.at[chunk, device],
            recv_sem=recv_sem.at[chunk, slot],
            device_id={"fft": device},
            device_id_type=MESH,
        )

    def keep(chunk):
        source, target = ends(chunk, me)
        return pltpu.make_async_copy(source, target, local_sem.at[2 + chunk])

    def post(chunk):
        def one(step, carry):
            remote(chunk, partner(chunk, step), me).start()
            return carry

        lax.fori_loop(1, partners(chunk), one, 0)
        keep(chunk).start()

    def collect(chunk):
        def one(step, carry):
            device = partner(chunk, partners(chunk) - step)
            remote(chunk, device, device).wait_recv()
            return carry

        lax.fori_loop(1, partners(chunk), one, 0)
        keep(chunk).wait()

    post(0)
    post(fields)
    post(1)

    matrix = table[...]
    half_matrix = table[pl.ds(pl.multiple_of(base * depth, members * depth), members * depth), :]
    load_psi.wait()
    load_pot.wait()

    def in_planes(index, carry):
        part = index // (bands * depth)
        band = index // depth % bands
        z = index % depth
        values = psi_v[part, band, z]
        local[band, part, z] = (
            multiply(matrix, values) + multiply(values, matrix) + pot_v[z] * values
        )
        return carry

    lax.fori_loop(0, parts * bands * depth, in_planes, 0)

    def load(ref, row):
        return ref.reshape(length * rows, length)[pl.ds(row, length, stride=rows), :]

    def store(ref, row, planes, values):
        ref.reshape(planes * rows, length)[pl.ds(row, planes, stride=rows), :] = values

    def once(field):
        band, part = divmod(field, parts)
        collect(field)
        for row in range(rows):
            values = load(psi_col.at[band, part], row)
            store(normal_col.at[band, part], row, length, multiply(matrix, values))
        post(fields + 1 + field)

    def twice(field):
        band, part = divmod(field, parts)
        planes = members * depth
        for row in range(rows):
            values = load(normal_col.at[band, part], row)
            values += load(pot_col, row) * load(psi_col.at[band, part], row)
            store(second_col.at[band, part], row, planes, multiply(half_matrix, values))
        post(2 * fields + 1 + field)

    def pot_copy(group, source):
        return pltpu.make_async_remote_copy(
            src_ref=pot_col.at[:, shared(0, source)],
            dst_ref=pot_col.at[:, shared(0, source)],
            send_sem=pot_send.at[group],
            recv_sem=pot_recv.at[group],
            device_id={"band": lax.rem(own + group, groups)},
            device_id_type=MESH,
        )

    def first_part(band):
        for part in range(parts):
            collect(fields + 1 + band * parts + part)

        def advance(z, carry):
            firsts = []
            seconds = []
            for part in range(parts):
                kinetic = normal[band, part, z]
                first = kinetic + local[band, part, z]
                both = kinetic + first
                firsts.append(first)
                seconds.append(
                    multiply(matrix, both) + multiply(both, matrix) + pot_v[z] * first
                )
            result[0, band, z] = psi_v[0, band, z] + TIME_STEP * firsts[1] - half * seconds[0]
            result[1, band, z] = psi_v[1, band, z] - TIME_STEP * firsts[0] - half * seconds[1]
            return carry

        lax.fori_loop(0, depth, advance, 0)

    def last_part(band):
        for part in range(parts):
            collect(2 * fields + 1 + band * parts + part)
        weight = occ[band]

        def finish(z, carry):
            real = result[0, band, z] - half * second[band, 0, z]
            imag = result[1, band, z] - half * second[band, 1, z]
            result[0, band, z] = real
            result[1, band, z] = imag
            share = weight * (real * real + imag * imag)
            partial[z] = share if band == 0 else partial[z] + share
            return carry

        lax.fori_loop(0, depth, finish, 0)

    once(0)
    post(2)
    collect(fields)
    for group in range(1, groups):
        pot_copy(group, own).start()
    once(1)
    for field in range(3, fields):
        post(field)
    for group in range(1, groups):
        pot_copy(group, lax.rem(own + groups - group, groups)).wait_recv()
    twice(0)
    twice(1)
    for field in range(2, fields - 1):
        once(field)
        twice(field)
    first_part(0)
    once(fields - 1)
    twice(fields - 1)
    last_part(0)
    for band in range(1, bands):
        first_part(band)
        last_part(band)

    def window_copies(group):
        target = lax.rem(own + group, groups)
        spans = (
            (lax.rem(target * width + length - EDGE, length), 0, EDGE),
            (target * width, EDGE, width),
            (lax.rem(target * width + width, length), EDGE + width, EDGE),
        )
        found = []
        for shift, z_from, z_to, planes in (
            (1, depth - 2, 0, 2), (slabs - 1, 0, depth + 2, 2), (0, 0, 2, depth),
        ):
            if shift == 0 and group == 0:
                continue
            there = {"fft": lax.rem(me + shift, slabs), "band": target}
            for x_from, x_to, size in spans:
                slot = len(found)
                found.append(pltpu.make_async_remote_copy(
                    src_ref=partial.at[pl.ds(z_from, planes), pl.ds(pl.multiple_of(x_from, EDGE), size)],
                    dst_ref=arrived.at[group, pl.ds(z_to, planes), pl.ds(x_to, size)],
                    send_sem=dens_send.at[group, slot],
                    recv_sem=dens_recv.at[group, slot],
                    device_id=there,
                    device_id_type=MESH,
                ))
        return found

    exchange = [copy for group in reversed(range(groups)) for copy in window_copies(group)]
    for copy in exchange:
        copy.start()
    write = pltpu.make_async_copy(result, out, local_sem.at[0])
    write.start()
    keep_window = []
    for slot, (x_from, x_to, size) in enumerate((
        (lax.rem(own * width + length - EDGE, length), 0, EDGE),
        (own * width, EDGE, width),
        (lax.rem(own * width + width, length), EDGE + width, EDGE),
    )):
        copy = pltpu.make_async_copy(
            partial.at[:, pl.ds(pl.multiple_of(x_from, EDGE), size)],
            arrived.at[0, pl.ds(2, depth), pl.ds(x_to, size)],
            dens_send.at[groups, slot],
        )
        copy.start()
        keep_window.append(copy)

    for chunk in range(3 * fields + 1):
        def drain(step, carry):
            remote(chunk, partner(chunk, step), me).wait_send()
            return carry

        lax.fori_loop(1, partners(chunk), drain, 0)
    for group in range(1, groups):
        pot_copy(group, own).wait_send()
    for copy in keep_window:
        copy.wait()
    for copy in exchange:
        copy.wait_recv()

    def total(z, carry):
        value = arrived[0, z]
        for group in range(1, groups):
            value += arrived[group, z]
        dens[z] = value
        return carry

    lax.fori_loop(0, depth + 4, total, 0)
    for copy in exchange:
        copy.wait_send()
    write.wait()


def step_in_kernel(wavefunctions, potential, occupation):
    parts, bands, depth, length, _ = wavefunctions.shape
    slabs, groups = (lax.axis_size("fft"), lax.axis_size("band"))
    rows, width = (2 * length // slabs, length // groups)
    table = jnp.asarray(second_derivative(length))
    chunks = 3 * bands * parts + 1
    by_band = pltpu.VMEM((bands, parts, depth, length, length), jnp.float32)
    by_part = pltpu.VMEM((parts, bands, depth, length, length), jnp.float32)
    columns = pltpu.VMEM((bands, parts, length, rows, length), jnp.float32)
    plane = (width + 2 * EDGE, length)
    result, padded = pl.pallas_call(
        functools.partial(step_kernel, slabs, groups),
        out_shape=(
            jax.ShapeDtypeStruct(wavefunctions.shape, jnp.float32),
            jax.ShapeDtypeStruct((depth + 4,) + plane, jnp.float32),
        ),
        in_specs=[
            pl.BlockSpec(memory_space=pl.ANY),
            pl.BlockSpec(memory_space=pl.ANY),
            pl.BlockSpec(memory_space=pltpu.SMEM),
            pl.BlockSpec(memory_space=pltpu.VMEM),
        ],
        out_specs=(
            pl.BlockSpec(memory_space=pl.ANY),
            pl.BlockSpec(memory_space=pltpu.VMEM),
        ),
        scratch_shapes=[
            by_part,
            pltpu.VMEM((depth, length, length), jnp.float32),
            columns,
            pltpu.VMEM((length, rows, length), jnp.float32),
            columns,
            pltpu.VMEM((bands, parts, length // 2, rows, length), jnp.float32),
            by_band,
            by_band,
            by_band,
            by_part,
            pltpu.VMEM((depth, length, length), jnp.float32),
            pltpu.VMEM((groups, depth + 4) + plane, jnp.float32),
            pltpu.SemaphoreType.DMA((chunks, slabs)),
            pltpu.SemaphoreType.DMA((chunks, slabs)),
            pltpu.SemaphoreType.DMA((chunks + 2,)),
            pltpu.SemaphoreType.DMA((groups + 1, 9)),
            pltpu.SemaphoreType.DMA((groups, 9)),
            pltpu.SemaphoreType.DMA((groups,)),
            pltpu.SemaphoreType.DMA((groups,)),
        ],
        compiler_params=pltpu.CompilerParams(
            collective_id=0, has_side_effects=True, vmem_limit_bytes=60 * 1024 * 1024
        ),
    )(wavefunctions, potential, occupation, table)
    return (result, padded[:, EDGE - 2 : EDGE + width + 2])


def per_device(wavefunctions, potential, occupation):
    _, _, depth, length, _ = wavefunctions.shape
    slabs, groups = (lax.axis_size("fft"), lax.axis_size("band"))
    share_rows = 2 * length // slabs // groups
    whole_tiles = slabs % 2 == 0 and groups == 2 and share_rows % 8 == 0
    step = step_in_kernel if whole_tiles else step_with_collectives
    result, padded = step(wavefunctions, potential, occupation)
    center = padded[2:-2, 2:-2]
    grad_z = fourth_order(padded[:, 2:-2], 0)
    grad_x = fourth_order(padded[2:-2], 1)
    grad_y = periodic_derivative(center, 2)
    reduced, energy = exchange_terms(center, grad_z, grad_x, grad_y)
    return (result, reduced, energy)


def solution(mesh):
    in_specs = (P(None, "band", "fft", None, None), P("fft", None, None), P("band"))
    out_specs = (P(None, "band", "fft", None, None), P("fft", "band", None), P("fft", "band", None))
    return jax.shard_map(
        per_device, mesh=mesh, in_specs=in_specs, out_specs=out_specs, check_vma=False
    )
```
